32 devices in a mesh: freq: 2 (over x), base: 4 (over y, core), pix: 4 (over z).
Axes of the slice: x: 2, y: 2, z: 4, core: 2. Of those that a mesh axis runs over, the one named last changes fastest.
Arguments:
- sensing_operator_parts: bfloat16 [2, 4096, 2048], P('freq', 'base', 'pix'), may hold values from -1 to 1
- sampled_correlations: float32 [64, 4096], P('freq', 'base'), may hold values from -40 to 40
- first_sky_estimate: float32 [64, 4, 4, 128], P('freq', 'pix', 'base'), may hold values from -2.5 to 2.5
- patch_order_record: int32 [6, 16], P(None, 'pix'), may hold values from 0 to 15, as said below
Outputs:
- image: float32 [64, 4, 4, 128], P('freq', 'pix', 'base')
The draws below stay inside these ranges and needn't reach their ends.
Inputs may be any that keep to these rules, and one draw needn't show every extreme that they name: `patch_order_record`: each row holds every tile number once; the tiles of rank under 4 are the same in every row.
All inputs are finite; a program needn't handle non-finite values.
Results may differ from the reference program's by a relative error of at most 0.0014.
Values may be sent and summed in bfloat16 or wider, within the bound.
A program may use at most 64 MiB of HBM per device.

```python
import math
import jax
import jax.numpy as jnp
from jax import lax

CH = 64
TILE = 128
ITERS = 6
TILES_DEV = 1
GROUPS = 2
TSH = 128
NP = 2048
NM = 4096
NT = 16
KEEP = 4
N_BASE = 4
N_PIX = 4


def draw_sensing_operator_parts(key, part):
    key_base, key_tile, key_col = jax.random.split(jax.random.fold_in(key, 11), 3)
    tile_scaling = jnp.exp(jax.random.uniform(key_tile, (GROUPS, 1, NT, 1), jnp.float32, math.log(0.3), math.log(1.5)))
    col_scale = jax.random.uniform(key_col, (GROUPS, 1, NT, TILE), jnp.float32, 0.7, 1.3)
    scales = (tile_scaling * col_scale).reshape(GROUPS, 1, NP)
    values = jnp.clip(jax.random.normal(key_base, (GROUPS, NM, NP), jnp.float32), -4.0, 4.0)
    denom = math.sqrt(NM) + math.sqrt(NP)
    return jnp.clip(values * scales / denom, -1.0, 1.0).astype(jnp.bfloat16)


def draw_sampled_correlations(key, part):
    key_main = jax.random.fold_in(jax.random.fold_in(key, 23), 0)
    chan_scale = jnp.exp(math.log(3.0) * jnp.arange(CH, dtype=jnp.float32) / max(CH - 1, 1))
    values = jnp.clip(jax.random.normal(key_main, (CH, NM), jnp.float32), -5.0, 5.0)
    return jnp.clip(values * chan_scale[:, None], -40.0, 40.0)


def draw_patch_order_record(key, part):
    key_set, key_rows = jax.random.split(jax.random.fold_in(key, 37))
    tile_order = jax.random.permutation(key_set, NT).astype(jnp.int32)
    all_rows = []
    for iteration in range(ITERS):
        key_kept, key_rest = jax.random.split(jax.random.fold_in(key_rows, iteration))
        kept_rank = jax.random.permutation(key_kept, KEEP).astype(jnp.int32)
        rest_rank = (KEEP + jax.random.permutation(key_rest, NT - KEEP)).astype(jnp.int32)
        rank_values = jnp.concatenate([kept_rank, rest_rank])
        rank_row = jnp.zeros((NT,), jnp.int32).at[tile_order].set(rank_values)
        all_rows.append(rank_row)
    return jnp.stack(all_rows)


def steps_of(key, shape, pieces, least, largest):
    gain = 1.0
    for axis_at, shards_of in pieces:
        heights = jax.random.uniform(jax.random.fold_in(jax.random.fold_in(key, 6), axis_at), (shards_of,), jnp.float32, least / len(pieces), largest / len(pieces))
        gain = gain * jnp.repeat(jnp.exp(heights), shape[axis_at] // shards_of).reshape((-1,) + (1,) * (len(shape) - 1 - axis_at))
    return gain


def noise(own_key, extent, width, limit, cuts=(), kind=jnp.bfloat16):
    result = width * jax.random.normal(own_key, extent, jnp.float32)
    if cuts:
        result = result * steps_of(own_key, extent, cuts, -0.22, 0.18)
    return jnp.clip(result, -limit, limit).astype(kind)


def setup_inputs(seed: int = 0) -> dict:
    key_of = jax.random.split(jax.random.key(seed), 5)
    return {
        "sensing_operator_parts": draw_sensing_operator_parts(jax.random.fold_in(key_of[4], 71), 0),
        "sampled_correlations": draw_sampled_correlations(jax.random.fold_in(key_of[4], 71), 0),
        "first_sky_estimate": noise(key_of[2], (CH, N_PIX, N_BASE, TSH), 1.0, 2.5, ((0, 2), (1, 4), (2, 4)), jnp.float32),
        "patch_order_record": draw_patch_order_record(jax.random.fold_in(key_of[4], 71), 0),
    }


descent_stride = 0.6
lam_shrink = 0.3
eps_norm = 1e-06

def reference(sensing_operator_parts, sampled_correlations, first_sky_estimate, patch_order_record):
    chan_grp = CH // GROUPS
    current = first_sky_estimate.reshape(CH, NP)
    for step in range(ITERS):
        rounded_amount = current.astype(jnp.bfloat16)
        grads = []
        for spectral_band_set in range(GROUPS):
            sensing_operator = sensing_operator_parts[spectral_band_set]
            part = rounded_amount[spectral_band_set * chan_grp:(spectral_band_set + 1) * chan_grp]
            pred = lax.dot_general(part, sensing_operator, (((1,), (1,)), ((), ())), preferred_element_type=jnp.float32)
            resid = (sampled_correlations[spectral_band_set * chan_grp:(spectral_band_set + 1) * chan_grp] - pred).astype(jnp.bfloat16)
            grads.append(jnp.dot(resid, sensing_operator, preferred_element_type=jnp.float32))
        moved = current + descent_stride * jnp.concatenate(grads, axis=0)
        tiles = moved.reshape(CH, NT, TILE)
        tnorm = lax.optimization_barrier(jnp.sum(tiles * tiles, axis=(0, 2)))
        rms_tile = jnp.sqrt(tnorm / (CH * TILE) + eps_norm)
        keeping = (patch_order_record[step] < KEEP).astype(jnp.float32)
        factor = keeping * rms_tile / (rms_tile + lam_shrink)
        current = (tiles * factor[None, :, None]).reshape(CH, NP)
    return current.reshape(CH, N_PIX, N_BASE, TILES_DEV * TILE)
```

```python
import functools

import jax
import jax.numpy as jnp
from jax import lax
from jax.experimental import pallas as pl
from jax.experimental.pallas import tpu as pltpu
from jax.sharding import PartitionSpec as P

CH = 64
ITERS = 6

descent_stride = 0.6
lam_shrink = 0.3
eps_norm = 1e-06

MESH = pl.DeviceIdType.MESH


def kernel(
    sizes,
    op_ref, meas_ref, sky_ref, rank_ref, out_ref,
    xr_buf, pred_buf, pred_in, resid_buf, resid_in, grad_buf, grad_in,
    z_buf, z_in, sq_buf, sq_in,
    x_send, x_recv, pred_send, pred_recv, resid_send, resid_recv,
    grad_send, grad_recv, sq_send, sq_recv,
):
    n_freq, n_base, n_pix, keep_count = sizes
    f = lax.axis_index("freq")
    b = lax.axis_index("base")
    p = lax.axis_index("pix")
    chans, share = sky_ref.shape
    width = op_ref.shape[0] // n_pix

    def base_at(o):
        return lax.rem(b + o + n_base, n_base)

    def pix_at(o):
        return lax.rem(p + o + n_pix, n_pix)

    def freq_at(o):
        return lax.rem(f + o, n_freq)

    barrier = pltpu.get_barrier_semaphore()
    greeted = 0
    for o in range(1, n_base):
        pl.semaphore_signal(barrier, inc=1, device_id={"base": base_at(o)}, device_id_type=MESH)
        greeted += 1
    for o in range(1, n_pix):
        pl.semaphore_signal(barrier, inc=1, device_id={"pix": pix_at(o)}, device_id_type=MESH)
        greeted += 1
    for fo in range(1, n_freq):
        for o in range(n_base):
            pl.semaphore_signal(
                barrier, inc=1, device_id={"freq": freq_at(fo), "base": base_at(o)}, device_id_type=MESH
            )
            greeted += 1
    pl.semaphore_wait(barrier, greeted)

    def share_copy(source, step, o):
        return pltpu.make_async_remote_copy(
            src_ref=source, dst_ref=z_in.at[step, o - 1],
            send_sem=x_send.at[o - 1], recv_sem=x_recv.at[step, o - 1],
            device_id={"base": base_at(o)}, device_id_type=MESH,
        )

    def sq_copy(step, fo, o):
        at = (fo - 1) * n_base + o
        return pltpu.make_async_remote_copy(
            src_ref=sq_buf, dst_ref=sq_in.at[step, at],
            send_sem=sq_send.at[at], recv_sem=sq_recv.at[step, at],
            device_id={"freq": freq_at(fo), "base": base_at(o)}, device_id_type=MESH,
        )

    def pred_copy(step, o):
        return pltpu.make_async_remote_copy(
            src_ref=pred_buf.at[o - 1], dst_ref=pred_in.at[step, o - 1],
            send_sem=pred_send.at[o - 1], recv_sem=pred_recv.at[step, o - 1],
            device_id={"pix": pix_at(o)}, device_id_type=MESH,
        )

    def resid_copy(step, o):
        return pltpu.make_async_remote_copy(
            src_ref=resid_buf, dst_ref=resid_in.at[step, o - 1],
            send_sem=resid_send.at[o - 1], recv_sem=resid_recv.at[step, o - 1],
            device_id={"pix": pix_at(o)}, device_id_type=MESH,
        )

    def grad_copy(step, o):
        return pltpu.make_async_remote_copy(
            src_ref=grad_buf.at[base_at(o)], dst_ref=grad_in.at[step, o - 1],
            send_sem=grad_send.at[o - 1], recv_sem=grad_recv.at[step, o - 1],
            device_id={"base": base_at(o)}, device_id_type=MESH,
        )

    def rows_of(at):
        return pl.ds(pl.multiple_of(at * width, width), width)

    if width % 128 == 0:
        own_meas = meas_ref[:, rows_of(p)]
    else:
        own_meas = jnp.zeros((chans, width), jnp.float32)
        for j in range(n_pix):
            own_meas = jnp.where(p == j, meas_ref[:, j * width:(j + 1) * width], own_meas)

    def squares(value):
        return jnp.sum((value * value).reshape(chans // 8, 8, share), axis=0)

    def factor_of(step, tile, total):
        rms = jnp.sqrt(jnp.sum(total, axis=(0, 1), keepdims=True) / (CH * share) + eps_norm)
        keeping = (rank_ref[step, tile] < keep_count).astype(jnp.float32)
        return keeping * rms / (rms + lam_shrink)

    order = sorted(range(1, n_pix), key=lambda o: -min(o, n_pix - o))

    def descend(step, current):
        rounded = jnp.concatenate([xr_buf[j] for j in range(n_base)], axis=1)

        def project(at):
            return lax.dot_general(
                rounded, op_ref[rows_of(at), :], (((1,), (1,)), ((), ())),
                preferred_element_type=jnp.float32,
            )

        for o in order:
            pred_buf[o - 1] = project(pix_at(o))
            pred_copy(step, o).start()
        total = project(p)
        for o in range(1, n_pix):
            pred_copy(step, o).wait()
            total = total + pred_in[step, o - 1]
        resid = (own_meas - total).astype(jnp.bfloat16)
        resid_buf[...] = resid
        for o in order:
            resid_copy(step, o).start()
        grad = jnp.dot(resid, op_ref[rows_of(p), :], preferred_element_type=jnp.float32)
        for o in range(1, n_pix):
            resid_copy(step, o).wait()
            grad = grad + jnp.dot(
                resid_in[step, o - 1], op_ref[rows_of(pix_at(-o)), :],
                preferred_element_type=jnp.float32,
            )
        for j in range(n_base):
            grad_buf[j] = grad[:, j * share:(j + 1) * share]
        for o in range(1, n_base):
            grad_copy(step, o).start()
        own = grad_buf[b]
        for o in range(1, n_base):
            grad_copy(step, o).wait()
            own = own + grad_in[step, o - 1]
        return current + descent_stride * own

    for o in range(1, n_base):
        share_copy(sky_ref, 0, o).start()
    first = sky_ref[...]
    xr_buf[b] = first.astype(jnp.bfloat16)
    for o in range(1, n_base):
        share_copy(sky_ref, 0, o).wait()
        xr_buf[base_at(-o)] = z_in[0, o - 1].astype(jnp.bfloat16)

    def iteration(step, current):
        moved = descend(step, current)
        z_buf[...] = moved
        own_sq = squares(moved)
        sq_buf[...] = own_sq
        for fo in range(1, n_freq):
            for o in reversed(range(n_base)):
                sq_copy(step, fo, o).start()
        for o in range(1, n_base):
            share_copy(z_buf, step + 1, o).start()
        result = None
        for o in range(n_base):
            if o:
                share_copy(z_buf, step + 1, o).wait()
                value = z_in[step + 1, o - 1]
                total = squares(value)
            else:
                value, total = moved, own_sq
            for fo in range(1, n_freq):
                sq_copy(step, fo, o).wait()
                total = total + sq_in[step, (fo - 1) * n_base + o]
            tile = base_at(-o)
            scaled = value * factor_of(step, tile, total)
            xr_buf[tile] = scaled.astype(jnp.bfloat16)
            if o == 0:
                result = scaled
        return result

    current = lax.fori_loop(0, ITERS - 1, iteration, first)
    last = ITERS - 1
    moved = descend(last, current)
    total = squares(moved)
    sq_buf[...] = total
    for fo in range(1, n_freq):
        sq_copy(last, fo, 0).start()
    for fo in range(1, n_freq):
        sq_copy(last, fo, 0).wait()
        total = total + sq_in[last, (fo - 1) * n_base]
    out_ref[...] = moved * factor_of(last, b, total)


def on_device(sensing_operator_parts, sampled_correlations, first_sky_estimate, patch_order_record):
    n_freq, n_base, n_pix = (lax.axis_size(a) for a in ("freq", "base", "pix"))
    chans = sampled_correlations.shape[0]
    share = first_sky_estimate.shape[3]
    op = sensing_operator_parts[0]
    rows, block = op.shape
    width = rows // n_pix
    keep_count = n_base * n_pix // 4
    f32, bf16 = jnp.float32, jnp.bfloat16
    dma = pltpu.SemaphoreType.DMA
    n_sq = (n_freq - 1) * n_base
    vmem = pl.BlockSpec(memory_space=pltpu.VMEM)
    result = pl.pallas_call(
        functools.partial(kernel, (n_freq, n_base, n_pix, keep_count)),
        out_shape=jax.ShapeDtypeStruct((chans, share), f32),
        in_specs=[vmem, vmem, vmem, pl.BlockSpec(memory_space=pltpu.SMEM)],
        out_specs=vmem,
        scratch_shapes=[
            pltpu.VMEM((n_base, chans, share), bf16),
            pltpu.VMEM((n_pix - 1, chans, width), f32),
            pltpu.VMEM((ITERS, n_pix - 1, chans, width), f32),
            pltpu.VMEM((chans, width), bf16),
            pltpu.VMEM((ITERS, n_pix - 1, chans, width), bf16),
            pltpu.VMEM((n_base, chans, share), f32),
            pltpu.VMEM((ITERS, n_base - 1, chans, share), f32),
            pltpu.VMEM((chans, share), f32),
            pltpu.VMEM((ITERS, n_base - 1, chans, share), f32),
            pltpu.VMEM((8, share), f32),
            pltpu.VMEM((ITERS, n_sq, 8, share), f32),
            dma((n_base - 1,)), dma((ITERS, n_base - 1)),
            dma((n_pix - 1,)), dma((ITERS, n_pix - 1)),
            dma((n_pix - 1,)), dma((ITERS, n_pix - 1)),
            dma((n_base - 1,)), dma((ITERS, n_base - 1)),
            dma((n_sq,)), dma((ITERS, n_sq)),
        ],
        compiler_params=pltpu.CompilerParams(collective_id=0, has_side_effects=True),
    )(op, sampled_correlations, first_sky_estimate.reshape(chans, share), patch_order_record)
    return result.reshape(chans, 1, 1, share)


def solution(mesh):
    in_specs = (
        P("freq", "base", "pix"),
        P("freq", "base"),
        P("freq", "pix", "base", None),
        P(None, "pix"),
    )
    out_specs = P("freq", "pix", "base", None)
    return jax.shard_map(
        on_device, mesh=mesh, in_specs=in_specs, out_specs=out_specs, check_vma=False
    )
```

```python
import functools

import jax
import jax.numpy as jnp
from jax import lax
from jax.experimental import pallas as pl
from jax.experimental.pallas import tpu as pltpu
from jax.sharding import PartitionSpec as P

CH = 64
ITERS = 6
PIECES = 2

descent_stride = 0.6
lam_shrink = 0.3
eps_norm = 1e-06

MESH = pl.DeviceIdType.MESH


def kernel(
    sizes,
    op_hbm, meas_ref, sky_ref, rank_ref, out_ref,
    op_ref, xr_buf, pred_buf, pred_in, grad_buf, grad_in,
    z_buf, z_in, sq_buf, sq_in,
    op_sem, x_send, x_recv, pred_send, pred_recv,
    grad_send, grad_recv, sq_send, sq_recv,
):
    n_freq, n_base, n_pix, keep_count = sizes
    f = lax.axis_index("freq")
    b = lax.axis_index("base")
    p = lax.axis_index("pix")
    chans, share = sky_ref.shape
    width = op_ref.shape[0] // PIECES

    def base_at(o):
        return lax.rem(b + o + n_base, n_base)

    def pix_at(o):
        return lax.rem(p + o + n_pix, n_pix)

    def freq_at(o):
        return lax.rem(f + o, n_freq)

    load = pltpu.make_async_copy(op_hbm, op_ref, op_sem)
    load.start()

    barrier = pltpu.get_barrier_semaphore()
    greeted = 0
    for o in range(1, n_base):
        pl.semaphore_signal(barrier, inc=1, device_id={"base": base_at(o)}, device_id_type=MESH)
        greeted += 1
    for o in range(1, n_pix):
        pl.semaphore_signal(barrier, inc=1, device_id={"pix": pix_at(o)}, device_id_type=MESH)
        greeted += 1
    for fo in range(1, n_freq):
        for o in range(n_base):
            pl.semaphore_signal(
                barrier, inc=1, device_id={"freq": freq_at(fo), "base": base_at(o)}, device_id_type=MESH
            )
            greeted += 1
    pl.semaphore_wait(barrier, greeted)

    def share_copy(source, step, o):
        return pltpu.make_async_remote_copy(
            src_ref=source, dst_ref=z_in.at[step, o - 1],
            send_sem=x_send.at[o - 1], recv_sem=x_recv.at[step, o - 1],
            device_id={"base": base_at(o)}, device_id_type=MESH,
        )

    def sq_copy(step, fo, o):
        at = (fo - 1) * n_base + o
        return pltpu.make_async_remote_copy(
            src_ref=sq_buf, dst_ref=sq_in.at[step, at],
            send_sem=sq_send.at[at], recv_sem=sq_recv.at[step, at],
            device_id={"freq": freq_at(fo), "base": base_at(o)}, device_id_type=MESH,
        )

    def pred_copy(step, h, o):
        at = h * (n_pix - 1) + o - 1
        return pltpu.make_async_remote_copy(
            src_ref=pred_buf.at[h], dst_ref=pred_in.at[step, at],
            send_sem=pred_send.at[at], recv_sem=pred_recv.at[step, at],
            device_id={"pix": pix_at(o)}, device_id_type=MESH,
        )

    def grad_copy(step, o):
        return pltpu.make_async_remote_copy(
            src_ref=grad_buf.at[base_at(o)], dst_ref=grad_in.at[step, o - 1],
            send_sem=grad_send.at[o - 1], recv_sem=grad_recv.at[step, o - 1],
            device_id={"base": base_at(o)}, device_id_type=MESH,
        )

    def squares(value):
        return jnp.sum((value * value).reshape(chans // 8, 8, share), axis=0)

    def factor_of(step, tile, total):
        rms = jnp.sqrt(jnp.sum(total, axis=(0, 1), keepdims=True) / (CH * share) + eps_norm)
        keeping = (rank_ref[tile, step] < keep_count).astype(jnp.float32)
        return keeping * rms / (rms + lam_shrink)

    order = sorted(range(1, n_pix), key=lambda o: -min(o, n_pix - o))

    def descend(step, current):
        rounded = jnp.concatenate([xr_buf[j] for j in range(n_base)], axis=1)

        pieces = []
        for h in range(PIECES):
            part = lax.dot_general(
                rounded, op_ref[h * width:(h + 1) * width, :], (((1,), (1,)), ((), ())),
                preferred_element_type=jnp.float32,
            )
            pred_buf[h] = part.astype(jnp.bfloat16)
            for o in order:
                pred_copy(step, h, o).start()
            pieces.append(part)
        grad = None
        for h in range(PIECES):
            total = meas_ref[:, h * width:(h + 1) * width] - pieces[h]
            for o in order[::-1]:
                pred_copy(step, h, o).wait()
                total = total - pred_in[step, h * (n_pix - 1) + o - 1].astype(jnp.float32)
            term = jnp.dot(
                total.astype(jnp.bfloat16), op_ref[h * width:(h + 1) * width, :],
                preferred_element_type=jnp.float32,
            )
            grad = term if grad is None else grad + term
        for j in range(n_base):
            grad_buf[j] = grad[:, j * share:(j + 1) * share]
        for o in range(1, n_base):
            grad_copy(step, o).start()
        own = grad_buf[b]
        for o in range(1, n_base):
            grad_copy(step, o).wait()
            own = own + grad_in[step, o - 1]
        return current + descent_stride * own

    for o in range(1, n_base):
        share_copy(sky_ref, 0, o).start()
    first = sky_ref[...]
    xr_buf[b] = first.astype(jnp.bfloat16)
    for o in range(1, n_base):
        share_copy(sky_ref, 0, o).wait()
        xr_buf[base_at(-o)] = z_in[0, o - 1].astype(jnp.bfloat16)
    load.wait()

    def iteration(step, current):
        moved = descend(step, current)
        z_buf[...] = moved
        own_sq = squares(moved)
        sq_buf[...] = own_sq
        for fo in range(1, n_freq):
            for o in reversed(range(n_base)):
                sq_copy(step, fo, o).start()
        for o in range(1, n_base):
            share_copy(z_buf, step + 1, o).start()
        result = None
        for o in range(n_base):
            if o:
                share_copy(z_buf, step + 1, o).wait()
                value = z_in[step + 1, o - 1]
                total = squares(value)
            else:
                value, total = moved, own_sq
            for fo in range(1, n_freq):
                sq_copy(step, fo, o).wait()
                total = total + sq_in[step, (fo - 1) * n_base + o]
            tile = base_at(-o)
            scaled = value * factor_of(step, tile, total)
            xr_buf[tile] = scaled.astype(jnp.bfloat16)
            if o == 0:
                result = scaled
        return result

    current = lax.fori_loop(0, ITERS - 1, iteration, first)
    last = ITERS - 1
    moved = descend(last, current)
    total = squares(moved)
    sq_buf[...] = total
    for fo in range(1, n_freq):
        sq_copy(last, fo, 0).start()
    for fo in range(1, n_freq):
        sq_copy(last, fo, 0).wait()
        total = total + sq_in[last, (fo - 1) * n_base]
    out_ref[...] = moved * factor_of(last, b, total)


def on_device(sensing_operator_parts, sampled_correlations, first_sky_estimate, patch_order_record):
    n_freq, n_base, n_pix = (lax.axis_size(a) for a in ("freq", "base", "pix"))
    chans = sampled_correlations.shape[0]
    share = first_sky_estimate.shape[3]
    op = sensing_operator_parts[0]
    rows, block = op.shape
    width = rows // PIECES
    n_pred = PIECES * (n_pix - 1)
    keep_count = n_base * n_pix // 4
    f32, bf16 = jnp.float32, jnp.bfloat16
    dma = pltpu.SemaphoreType.DMA
    n_sq = (n_freq - 1) * n_base
    vmem = pl.BlockSpec(memory_space=pltpu.VMEM)
    result = pl.pallas_call(
        functools.partial(kernel, (n_freq, n_base, n_pix, keep_count)),
        out_shape=jax.ShapeDtypeStruct((chans, share), f32),
        in_specs=[pl.BlockSpec(memory_space=pl.ANY), vmem, vmem, pl.BlockSpec(memory_space=pltpu.SMEM)],
        out_specs=vmem,
        scratch_shapes=[
            pltpu.VMEM((rows, block), bf16),
            pltpu.VMEM((n_base, chans, share), bf16),
            pltpu.VMEM((PIECES, chans, width), bf16),
            pltpu.VMEM((ITERS, n_pred, chans, width), bf16),
            pltpu.VMEM((n_base, chans, share), f32),
            pltpu.VMEM((ITERS, n_base - 1, chans, share), f32),
            pltpu.VMEM((chans, share), f32),
            pltpu.VMEM((ITERS, n_base - 1, chans, share), f32),
            pltpu.VMEM((8, share), f32),
            pltpu.VMEM((ITERS, n_sq, 8, share), f32),
            dma, dma((n_base - 1,)), dma((ITERS, n_base - 1)),
            dma((n_pred,)), dma((ITERS, n_pred)),
            dma((n_base - 1,)), dma((ITERS, n_base - 1)),
            dma((n_sq,)), dma((ITERS, n_sq)),
        ],
        compiler_params=pltpu.CompilerParams(collective_id=0, has_side_effects=True),
    )(op, sampled_correlations, first_sky_estimate.reshape(chans, share), patch_order_record.T)
    return result.reshape(chans, 1, 1, share)


def solution(mesh):
    in_specs = (
        P("freq", "base", "pix"),
        P("freq", "base"),
        P("freq", "pix", "base", None),
        P(None, "pix"),
    )
    out_specs = P("freq", "pix", "base", None)
    return jax.shard_map(
        on_device, mesh=mesh, in_specs=in_specs, out_specs=out_specs, check_vma=False
    )
```

```python
import functools

import jax
import jax.numpy as jnp
from jax import lax
from jax.experimental import pallas as pl
from jax.experimental.pallas import tpu as pltpu
from jax.sharding import PartitionSpec as P

CH = 64
ITERS = 6

descent_stride = 0.6
lam_shrink = 0.3
eps_norm = 1e-06

MESH = pl.DeviceIdType.MESH


def kernel(
    sizes,
    op_hbm, meas_ref, sky_ref, rank_ref, out_ref, factor_ref,
    op_ref, xr_buf, grad_buf, grad_in,
    z_buf, z_in, sq_buf, sq_in,
    op_sem, x_send, x_recv,
    grad_send, grad_recv, sq_send, sq_recv,
    merge_buf, *piece_scratch,
):
    n_freq, n_base, n_pix, keep_count, pieces = sizes
    pred_buf, pred_in, pred_send, pred_recv = (piece_scratch[i::4] for i in range(4))
    f = lax.axis_index("freq")
    b = lax.axis_index("base")
    p = lax.axis_index("pix")
    chans, share = sky_ref.shape

    def base_at(o):
        return lax.rem(b + o + n_base, n_base)

    def pix_at(o):
        return lax.rem(p + o + n_pix, n_pix)

    def freq_at(o):
        return lax.rem(f + o, n_freq)

    load = pltpu.make_async_copy(op_hbm, op_ref, op_sem)
    load.start()

    barrier = pltpu.get_barrier_semaphore()
    greeted = 0
    for o in range(1, n_base):
        pl.semaphore_signal(barrier, inc=1, device_id={"base": base_at(o)}, device_id_type=MESH)
        greeted += 1
    for o in range(1, n_pix):
        pl.semaphore_signal(barrier, inc=1, device_id={"pix": pix_at(o)}, device_id_type=MESH)
        greeted += 1
    for fo in range(1, n_freq):
        for o in range(n_base):
            pl.semaphore_signal(
                barrier, inc=1, device_id={"freq": freq_at(fo), "base": base_at(o)}, device_id_type=MESH
            )
            greeted += 1
    pl.semaphore_wait(barrier, greeted)

    def share_copy(source, step, o):
        return pltpu.make_async_remote_copy(
            src_ref=source, dst_ref=z_in.at[step, o - 1],
            send_sem=x_send.at[o - 1], recv_sem=x_recv.at[step, o - 1],
            device_id={"base": base_at(o)}, device_id_type=MESH,
        )

    def sq_copy(step, fo, o):
        at = (fo - 1) * n_base + o
        return pltpu.make_async_remote_copy(
            src_ref=sq_buf, dst_ref=sq_in.at[step, at],
            send_sem=sq_send.at[at], recv_sem=sq_recv.at[step, at],
            device_id={"freq": freq_at(fo), "base": base_at(o)}, device_id_type=MESH,
        )

    def pred_copy(step, h, o):
        return pltpu.make_async_remote_copy(
            src_ref=pred_buf[h], dst_ref=pred_in[h].at[step, o - 1],
            send_sem=pred_send[h].at[o - 1], recv_sem=pred_recv[h].at[step, o - 1],
            device_id={"pix": pix_at(o)}, device_id_type=MESH,
        )

    beside = p + 1 - 2 * lax.rem(p, 2)
    across = 3 - p
    inner = jnp.logical_or(p == 1, p == 2)

    def pair_copy(step):
        return pltpu.make_async_remote_copy(
            src_ref=pred_buf[0], dst_ref=pred_in[0].at[step, 0],
            send_sem=pred_send[0].at[0], recv_sem=pred_recv[0].at[step, 0],
            device_id={"pix": beside}, device_id_type=MESH,
        )

    def merged_copy(step, k):
        target = across + 1 - 2 * lax.rem(across, 2) if k else across
        return pltpu.make_async_remote_copy(
            src_ref=merge_buf, dst_ref=pred_in[0].at[step, 1],
            send_sem=pred_send[0].at[1 + k], recv_sem=pred_recv[0].at[step, 1],
            device_id={"pix": target}, device_id_type=MESH,
        )

    def grad_copy(step, o):
        return pltpu.make_async_remote_copy(
            src_ref=grad_buf.at[base_at(o)], dst_ref=grad_in.at[step, o - 1],
            send_sem=grad_send.at[o - 1], recv_sem=grad_recv.at[step, o - 1],
            device_id={"base": base_at(o)}, device_id_type=MESH,
        )

    def squares(value):
        return jnp.sum((value * value).reshape(chans // 8, 8, share), axis=0)

    def factor_of(step, tile, total):
        rms = jnp.sqrt(jnp.sum(total, axis=(0, 1), keepdims=True) / (CH * share) + eps_norm)
        keeping = (rank_ref[tile, step] < keep_count).astype(jnp.float32)
        return keeping * rms / (rms + lam_shrink)

    order = sorted(range(1, n_pix), key=lambda o: -min(o, n_pix - o))

    def descend(step, current):
        rounded = jnp.concatenate([xr_buf[j] for j in range(n_base)], axis=1)

        parts = []
        for h, (start, width, merged) in enumerate(pieces):
            part = lax.dot_general(
                rounded, op_ref[start:start + width, :], (((1,), (1,)), ((), ())),
                preferred_element_type=jnp.float32,
            )
            pred_buf[h][...] = part.astype(jnp.bfloat16)
            if merged:
                pair_copy(step).start()
            else:
                for o in order:
                    pred_copy(step, h, o).start()
            parts.append(part)
        if pieces[0][2]:
            pair_copy(step).wait()
            parts[0] = parts[0] + pred_in[0][step, 0].astype(jnp.float32)
            merge_buf[...] = parts[0].astype(jnp.bfloat16)

            @pl.when(inner)
            def _():
                for k in (1, 0):
                    merged_copy(step, k).start()

        grad = None
        for h in [*range(1, len(pieces)), 0] if pieces[0][2] else range(len(pieces)):
            start, width, merged = pieces[h]
            total = meas_ref[:, start:start + width] - parts[h]
            if merged:
                merged_copy(step, 0).wait_recv()
                total = total - pred_in[h][step, 1].astype(jnp.float32)

                @pl.when(inner)
                def _():
                    for k in (0, 1):
                        merged_copy(step, k).wait_send()
            else:
                for o in order[::-1]:
                    pred_copy(step, h, o).wait()
                    total = total - pred_in[h][step, o - 1].astype(jnp.float32)
            term = jnp.dot(
                total.astype(jnp.bfloat16), op_ref[start:start + width, :],
                preferred_element_type=jnp.float32,
            )
            grad = term if grad is None else grad + term
        for j in range(n_base):
            grad_buf[j] = grad[:, j * share:(j + 1) * share]
        for o in range(1, n_base):
            grad_copy(step, o).start()
        own = grad_buf[b]
        for o in range(1, n_base):
            grad_copy(step, o).wait()
            own = own + grad_in[step, o - 1]
        return current + descent_stride * own

    for o in range(1, n_base):
        share_copy(sky_ref, 0, o).start()
    first = sky_ref[...]
    xr_buf[b] = first.astype(jnp.bfloat16)
    for o in range(1, n_base):
        share_copy(sky_ref, 0, o).wait()
        xr_buf[base_at(-o)] = z_in[0, o - 1].astype(jnp.bfloat16)
    load.wait()

    def iteration(step, current):
        moved = descend(step, current)
        z_buf[...] = moved
        own_sq = squares(moved)
        sq_buf[...] = own_sq
        for fo in range(1, n_freq):
            for o in reversed(range(n_base)):
                sq_copy(step, fo, o).start()
        for o in range(1, n_base):
            share_copy(z_buf, step + 1, o).start()
        result = None
        for o in range(n_base):
            if o:
                share_copy(z_buf, step + 1, o).wait()
                value = z_in[step + 1, o - 1]
                total = squares(value)
            else:
                value, total = moved, own_sq
            for fo in range(1, n_freq):
                sq_copy(step, fo, o).wait()
                total = total + sq_in[step, (fo - 1) * n_base + o]
            tile = base_at(-o)
            scaled = value * factor_of(step, tile, total)
            xr_buf[tile] = scaled.astype(jnp.bfloat16)
            if o == 0:
                result = scaled
        return result

    current = lax.fori_loop(0, ITERS - 1, iteration, first)
    last = ITERS - 1
    moved = descend(last, current)
    total = squares(moved)
    sq_buf[...] = total
    for fo in range(1, n_freq):
        sq_copy(last, fo, 0).start()
    for fo in range(1, n_freq):
        sq_copy(last, fo, 0).wait()
        total = total + sq_in[last, (fo - 1) * n_base]
    out_ref[...] = moved
    factor_ref[...] = jnp.broadcast_to(factor_of(last, b, total), factor_ref.shape)


def on_device(sensing_operator_parts, sampled_correlations, first_sky_estimate, patch_order_record):
    n_freq, n_base, n_pix = (lax.axis_size(a) for a in ("freq", "base", "pix"))
    chans = sampled_correlations.shape[0]
    share = first_sky_estimate.shape[3]
    op = sensing_operator_parts[0]
    rows, block = op.shape
    f32, bf16 = jnp.float32, jnp.bfloat16
    dma = pltpu.SemaphoreType.DMA
    if n_pix == 4 and rows % 1024 == 0:
        eighth = rows // 8
        pieces = ((0, 3 * eighth, True), (3 * eighth, 2 * eighth, False), (5 * eighth, 3 * eighth, False))
    else:
        pieces = tuple((h * rows // 2, rows // 2, False) for h in range(2))
    piece_scratch = []
    for _, width, _ in pieces:
        piece_scratch += [
            pltpu.VMEM((chans, width), bf16),
            pltpu.VMEM((ITERS, n_pix - 1, chans, width), bf16),
            dma((n_pix - 1,)), dma((ITERS, n_pix - 1)),
        ]
    keep_count = n_base * n_pix // 4
    n_sq = (n_freq - 1) * n_base
    vmem = pl.BlockSpec(memory_space=pltpu.VMEM)
    moved, factor = pl.pallas_call(
        functools.partial(kernel, (n_freq, n_base, n_pix, keep_count, pieces)),
        out_shape=[jax.ShapeDtypeStruct((chans, share), f32), jax.ShapeDtypeStruct((1, share), f32)],
        in_specs=[pl.BlockSpec(memory_space=pl.ANY), vmem, vmem, pl.BlockSpec(memory_space=pltpu.SMEM)],
        out_specs=[vmem, vmem],
        scratch_shapes=[
            pltpu.VMEM((rows, block), bf16),
            pltpu.VMEM((n_base, chans, share), bf16),
            pltpu.VMEM((n_base, chans, share), f32),
            pltpu.VMEM((ITERS, n_base - 1, chans, share), f32),
            pltpu.VMEM((chans, share), f32),
            pltpu.VMEM((ITERS, n_base - 1, chans, share), f32),
            pltpu.VMEM((8, share), f32),
            pltpu.VMEM((ITERS, n_sq, 8, share), f32),
            dma, dma((n_base - 1,)), dma((ITERS, n_base - 1)),
            dma((n_base - 1,)), dma((ITERS, n_base - 1)),
            dma((n_sq,)), dma((ITERS, n_sq)),
            pltpu.VMEM((chans, pieces[0][1]), bf16),
            *piece_scratch,
        ],
        compiler_params=pltpu.CompilerParams(collective_id=0, has_side_effects=True),
    )(op, sampled_correlations, first_sky_estimate.reshape(chans, share), patch_order_record.T)
    return (moved * factor).reshape(chans, 1, 1, share)


def solution(mesh):
    in_specs = (
        P("freq", "base", "pix"),
        P("freq", "base"),
        P("freq", "pix", "base", None),
        P(None, "pix"),
    )
    out_specs = P("freq", "pix", "base", None)
    return jax.shard_map(
        on_device, mesh=mesh, in_specs=in_specs, out_specs=out_specs, check_vma=False
    )
```

```python
import functools

import jax
import jax.numpy as jnp
from jax import lax
from jax.experimental import pallas as pl
from jax.experimental.pallas import tpu as pltpu
from jax.sharding import PartitionSpec as P

CH = 64
ITERS = 6

descent_stride = 0.6
lam_shrink = 0.3
eps_norm = 1e-06

MESH = pl.DeviceIdType.MESH


def kernel(
    sizes,
    op_hbm, meas_ref, sky_ref, rank_ref, out_ref,
    op_ref, xr_buf, grad_buf, grad_in,
    z_buf, z_in, sq_buf, sq_in,
    op_sem, x_send, x_recv,
    grad_send, grad_recv, sq_send, sq_recv,
    merge_buf, *piece_scratch,
):
    n_freq, n_base, n_pix, keep_count, pieces = sizes
    pred_buf, pred_in, pred_send, pred_recv = (piece_scratch[i::4] for i in range(4))
    f = lax.axis_index("freq")
    b = lax.axis_index("base")
    p = lax.axis_index("pix")
    chans, share = sky_ref.shape

    def base_at(o):
        return lax.rem(b + o + n_base, n_base)

    def pix_at(o):
        return lax.rem(p + o + n_pix, n_pix)

    def freq_at(o):
        return lax.rem(f + o, n_freq)

    load = pltpu.make_async_copy(op_hbm, op_ref, op_sem)
    load.start()

    barrier = pltpu.get_barrier_semaphore()
    greeted = 0
    for o in range(1, n_base):
        pl.semaphore_signal(barrier, inc=1, device_id={"base": base_at(o)}, device_id_type=MESH)
        greeted += 1
    for o in range(1, n_pix):
        pl.semaphore_signal(barrier, inc=1, device_id={"pix": pix_at(o)}, device_id_type=MESH)
        greeted += 1
    for fo in range(1, n_freq):
        for o in range(n_base):
            pl.semaphore_signal(
                barrier, inc=1, device_id={"freq": freq_at(fo), "base": base_at(o)}, device_id_type=MESH
            )
            greeted += 1
    pl.semaphore_wait(barrier, greeted)

    def share_copy(source, step, o):
        return pltpu.make_async_remote_copy(
            src_ref=source, dst_ref=z_in.at[step, o - 1],
            send_sem=x_send.at[o - 1], recv_sem=x_recv.at[step, o - 1],
            device_id={"base": base_at(o)}, device_id_type=MESH,
        )

    def sq_copy(step, fo, o):
        at = (fo - 1) * n_base + o
        return pltpu.make_async_remote_copy(
            src_ref=sq_buf, dst_ref=sq_in.at[step, at],
            send_sem=sq_send.at[at], recv_sem=sq_recv.at[step, at],
            device_id={"freq": freq_at(fo), "base": base_at(o)}, device_id_type=MESH,
        )

    def pred_copy(step, h, o):
        return pltpu.make_async_remote_copy(
            src_ref=pred_buf[h], dst_ref=pred_in[h].at[step, o - 1],
            send_sem=pred_send[h].at[o - 1], recv_sem=pred_recv[h].at[step, o - 1],
            device_id={"pix": pix_at(o)}, device_id_type=MESH,
        )

    beside = p + 1 - 2 * lax.rem(p, 2)
    across = 3 - p
    inner = jnp.logical_or(p == 1, p == 2)

    def pair_copy(step):
        return pltpu.make_async_remote_copy(
            src_ref=pred_buf[0], dst_ref=pred_in[0].at[step, 0],
            send_sem=pred_send[0].at[0], recv_sem=pred_recv[0].at[step, 0],
            device_id={"pix": beside}, device_id_type=MESH,
        )

    def merged_copy(step, k):
        target = across + 1 - 2 * lax.rem(across, 2) if k else across
        return pltpu.make_async_remote_copy(
            src_ref=merge_buf, dst_ref=pred_in[0].at[step, 1],
            send_sem=pred_send[0].at[1 + k], recv_sem=pred_recv[0].at[step, 1],
            device_id={"pix": target}, device_id_type=MESH,
        )

    def grad_copy(step, o):
        return pltpu.make_async_remote_copy(
            src_ref=grad_buf.at[base_at(o)], dst_ref=grad_in.at[step, o - 1],
            send_sem=grad_send.at[o - 1], recv_sem=grad_recv.at[step, o - 1],
            device_id={"base": base_at(o)}, device_id_type=MESH,
        )

    def squares(value):
        return jnp.sum((value * value).reshape(chans // 8, 8, share), axis=0)

    def factor_of(step, tile, total):
        rms = jnp.sqrt(jnp.sum(total, axis=(0, 1), keepdims=True) / (CH * share) + eps_norm)
        keeping = (rank_ref[tile, step] < keep_count).astype(jnp.float32)
        return keeping * rms / (rms + lam_shrink)

    order = sorted(range(1, n_pix), key=lambda o: -min(o, n_pix - o))

    def descend(step, current):
        rounded = jnp.concatenate([xr_buf[j] for j in range(n_base)], axis=1)

        parts = []
        for h, (start, width, merged) in enumerate(pieces):
            part = lax.dot_general(
                rounded, op_ref[start:start + width, :], (((1,), (1,)), ((), ())),
                preferred_element_type=jnp.float32,
            )
            pred_buf[h][...] = part.astype(jnp.bfloat16)
            if merged:
                pair_copy(step).start()
            else:
                for o in order:
                    pred_copy(step, h, o).start()
            parts.append(part)
        if pieces[0][2]:
            pair_copy(step).wait_recv()
            parts[0] = parts[0] + pred_in[0][step, 0].astype(jnp.float32)
            merge_buf[...] = parts[0].astype(jnp.bfloat16)

            @pl.when(inner)
            def _():
                for k in (1, 0):
                    merged_copy(step, k).start()

        grad = None
        for h in [*range(1, len(pieces)), 0] if pieces[0][2] else range(len(pieces)):
            start, width, merged = pieces[h]
            total = meas_ref[:, start:start + width] - parts[h]
            if merged:
                merged_copy(step, 0).wait_recv()
                total = total - pred_in[h][step, 1].astype(jnp.float32)
            else:
                for o in order[::-1]:
                    pred_copy(step, h, o).wait_recv()
                    total = total - pred_in[h][step, o - 1].astype(jnp.float32)
            term = jnp.dot(
                total.astype(jnp.bfloat16), op_ref[start:start + width, :],
                preferred_element_type=jnp.float32,
            )
            grad = term if grad is None else grad + term
        for j in range(n_base):
            grad_buf[j] = grad[:, j * share:(j + 1) * share]
        for o in range(1, n_base):
            grad_copy(step, o).start()
        own = grad_buf[b]
        for o in range(1, n_base):
            grad_copy(step, o).wait_recv()
            own = own + grad_in[step, o - 1]
        return current + descent_stride * own

    def drain(step):
        for h, (_, _, merged) in enumerate(pieces):
            if merged:
                pair_copy(step).wait_send()

                @pl.when(inner)
                def _():
                    for k in (0, 1):
                        merged_copy(step, k).wait_send()
            else:
                for o in order:
                    pred_copy(step, h, o).wait_send()
        for o in range(1, n_base):
            grad_copy(step, o).wait_send()

    for o in range(1, n_base):
        share_copy(sky_ref, 0, o).start()
    first = sky_ref[...]
    xr_buf[b] = first.astype(jnp.bfloat16)
    for o in range(1, n_base):
        share_copy(sky_ref, 0, o).wait()
        xr_buf[base_at(-o)] = z_in[0, o - 1].astype(jnp.bfloat16)
    load.wait()

    def iteration(step, current):
        moved = descend(step, current)
        z_buf[...] = moved
        own_sq = squares(moved)
        sq_buf[...] = own_sq
        for fo in range(1, n_freq):
            for o in reversed(range(n_base)):
                sq_copy(step, fo, o).start()
        for o in range(1, n_base):
            share_copy(z_buf, step + 1, o).start()
        drain(step)
        result = None
        for o in range(n_base):
            if o:
                share_copy(z_buf, step + 1, o).wait_recv()
                value = z_in[step + 1, o - 1]
                total = squares(value)
            else:
                value, total = moved, own_sq
            for fo in range(1, n_freq):
                sq_copy(step, fo, o).wait_recv()
                total = total + sq_in[step, (fo - 1) * n_base + o]
            tile = base_at(-o)
            scaled = value * factor_of(step, tile, total)
            xr_buf[tile] = scaled.astype(jnp.bfloat16)
            if o == 0:
                result = scaled
        for o in range(1, n_base):
            share_copy(z_buf, step + 1, o).wait_send()
        for fo in range(1, n_freq):
            for o in range(n_base):
                sq_copy(step, fo, o).wait_send()
        return result

    current = lax.fori_loop(0, ITERS - 1, iteration, first)
    last = ITERS - 1
    moved = descend(last, current)
    total = squares(moved)
    sq_buf[...] = total
    for fo in range(1, n_freq):
        sq_copy(last, fo, 0).start()
    drain(last)
    for fo in range(1, n_freq):
        sq_copy(last, fo, 0).wait()
        total = total + sq_in[last, (fo - 1) * n_base]
    out_ref[...] = moved * factor_of(last, b, total)


def on_device(sensing_operator_parts, sampled_correlations, first_sky_estimate, patch_order_record):
    n_freq, n_base, n_pix = (lax.axis_size(a) for a in ("freq", "base", "pix"))
    chans = sampled_correlations.shape[0]
    share = first_sky_estimate.shape[3]
    op = sensing_operator_parts[0]
    rows, block = op.shape
    f32, bf16 = jnp.float32, jnp.bfloat16
    dma = pltpu.SemaphoreType.DMA
    if n_pix == 4 and rows % 1024 == 0:
        eighth = rows // 8
        pieces = ((0, 3 * eighth, True), (3 * eighth, 2 * eighth, False), (5 * eighth, 3 * eighth, False))
    else:
        pieces = tuple((h * rows // 2, rows // 2, False) for h in range(2))
    piece_scratch = []
    for _, width, _ in pieces:
        piece_scratch += [
            pltpu.VMEM((chans, width), bf16),
            pltpu.VMEM((ITERS, n_pix - 1, chans, width), bf16),
            dma((n_pix - 1,)), dma((ITERS, n_pix - 1)),
        ]
    keep_count = n_base * n_pix // 4
    n_sq = (n_freq - 1) * n_base
    vmem = pl.BlockSpec(memory_space=pltpu.VMEM)
    result = pl.pallas_call(
        functools.partial(kernel, (n_freq, n_base, n_pix, keep_count, pieces)),
        out_shape=jax.ShapeDtypeStruct((chans, share), f32),
        in_specs=[pl.BlockSpec(memory_space=pl.ANY), vmem, vmem, pl.BlockSpec(memory_space=pltpu.SMEM)],
        out_specs=vmem,
        scratch_shapes=[
            pltpu.VMEM((rows, block), bf16),
            pltpu.VMEM((n_base, chans, share), bf16),
            pltpu.VMEM((n_base, chans, share), f32),
            pltpu.VMEM((ITERS, n_base - 1, chans, share), f32),
            pltpu.VMEM((chans, share), f32),
            pltpu.VMEM((ITERS, n_base - 1, chans, share), f32),
            pltpu.VMEM((8, share), f32),
            pltpu.VMEM((ITERS, n_sq, 8, share), f32),
            dma, dma((n_base - 1,)), dma((ITERS, n_base - 1)),
            dma((n_base - 1,)), dma((ITERS, n_base - 1)),
            dma((n_sq,)), dma((ITERS, n_sq)),
            pltpu.VMEM((chans, pieces[0][1]), bf16),
            *piece_scratch,
        ],
        compiler_params=pltpu.CompilerParams(collective_id=0, has_side_effects=True),
    )(op, sampled_correlations, first_sky_estimate.reshape(chans, share), patch_order_record.T)
    return result.reshape(chans, 1, 1, share)


def solution(mesh):
    in_specs = (
        P("freq", "base", "pix"),
        P("freq", "base"),
        P("freq", "pix", "base", None),
        P(None, "pix"),
    )
    out_specs = P("freq", "pix", "base", None)
    return jax.shard_map(
        on_device, mesh=mesh, in_specs=in_specs, out_specs=out_specs, check_vma=False
    )
```

```python
import functools

import jax
import jax.numpy as jnp
from jax import lax
from jax.experimental import pallas as pl
from jax.experimental.pallas import tpu as pltpu
from jax.sharding import PartitionSpec as P

CH = 64
ITERS = 6

descent_stride = 0.6
lam_shrink = 0.3
eps_norm = 1e-06

MESH = pl.DeviceIdType.MESH


def kernel(
    sizes,
    op_hbm, meas_ref, sky_ref, rank_ref, out_ref,
    op_ref, xr_buf, grad_buf, grad_in,
    z_buf, z_in, sq_buf, sq_in,
    op_sem, x_send, x_recv,
    grad_send, grad_recv, sq_send, sq_recv,
    merge_buf, *piece_scratch,
):
    n_freq, n_base, n_pix, keep_count, pieces = sizes
    pred_buf, pred_in, pred_send, pred_recv = (piece_scratch[i::4] for i in range(4))
    f = lax.axis_index("freq")
    b = lax.axis_index("base")
    p = lax.axis_index("pix")
    chans, share = sky_ref.shape

    def base_at(o):
        return lax.rem(b + o + n_base, n_base)

    def pix_at(o):
        return lax.rem(p + o + n_pix, n_pix)

    def freq_at(o):
        return lax.rem(f + o, n_freq)

    load = pltpu.make_async_copy(op_hbm, op_ref, op_sem)
    load.start()

    barrier = pltpu.get_barrier_semaphore()
    greeted = 0
    for o in range(1, n_base):
        pl.semaphore_signal(barrier, inc=1, device_id={"base": base_at(o)}, device_id_type=MESH)
        greeted += 1
    for o in range(1, n_pix):
        pl.semaphore_signal(barrier, inc=1, device_id={"pix": pix_at(o)}, device_id_type=MESH)
        greeted += 1
    for fo in range(1, n_freq):
        for o in range(n_base):
            pl.semaphore_signal(
                barrier, inc=1, device_id={"freq": freq_at(fo), "base": base_at(o)}, device_id_type=MESH
            )
            greeted += 1
    pl.semaphore_wait(barrier, greeted)

    def share_copy(source, step, o):
        return pltpu.make_async_remote_copy(
            src_ref=source, dst_ref=z_in.at[step, o - 1],
            send_sem=x_send.at[o - 1], recv_sem=x_recv.at[step, o - 1],
            device_id={"base": base_at(o)}, device_id_type=MESH,
        )

    def sq_copy(step, fo, o):
        at = (fo - 1) * n_base + o
        return pltpu.make_async_remote_copy(
            src_ref=sq_buf, dst_ref=sq_in.at[step, at],
            send_sem=sq_send.at[at], recv_sem=sq_recv.at[step, at],
            device_id={"freq": freq_at(fo), "base": base_at(o)}, device_id_type=MESH,
        )

    def pred_copy(step, h, o):
        return pltpu.make_async_remote_copy(
            src_ref=pred_buf[h], dst_ref=pred_in[h].at[step, o - 1],
            send_sem=pred_send[h].at[o - 1], recv_sem=pred_recv[h].at[step, o - 1],
            device_id={"pix": pix_at(o)}, device_id_type=MESH,
        )

    beside = p + 1 - 2 * lax.rem(p, 2)
    across = 3 - p
    inner = jnp.logical_or(p == 1, p == 2)

    def pair_copy(step):
        return pltpu.make_async_remote_copy(
            src_ref=pred_buf[0], dst_ref=pred_in[0].at[step, 0],
            send_sem=pred_send[0].at[0], recv_sem=pred_recv[0].at[step, 0],
            device_id={"pix": beside}, device_id_type=MESH,
        )

    def merged_copy(step, k):
        target = across + 1 - 2 * lax.rem(across, 2) if k else across
        return pltpu.make_async_remote_copy(
            src_ref=merge_buf, dst_ref=pred_in[0].at[step, 1],
            send_sem=pred_send[0].at[1 + k], recv_sem=pred_recv[0].at[step, 1],
            device_id={"pix": target}, device_id_type=MESH,
        )

    def grad_copy(step, o):
        return pltpu.make_async_remote_copy(
            src_ref=grad_buf.at[base_at(o)], dst_ref=grad_in.at[step, o - 1],
            send_sem=grad_send.at[o - 1], recv_sem=grad_recv.at[step, o - 1],
            device_id={"base": base_at(o)}, device_id_type=MESH,
        )

    def squares(value):
        return jnp.sum(value * value, axis=0, keepdims=True)

    def factor_of(step, tile, total):
        rms = jnp.sqrt(jnp.sum(total, axis=(0, 1), keepdims=True) / (CH * share) + eps_norm)
        keeping = (rank_ref[tile, step] < keep_count).astype(jnp.float32)
        return keeping * rms / (rms + lam_shrink)

    order = sorted(range(1, n_pix), key=lambda o: -min(o, n_pix - o))

    def descend(step, current):
        rounded = jnp.concatenate([xr_buf[j] for j in range(n_base)], axis=1)

        parts = []
        for h, (start, width, merged) in enumerate(pieces):
            part = lax.dot_general(
                rounded, op_ref[start:start + width, :], (((1,), (1,)), ((), ())),
                preferred_element_type=jnp.float32,
            )
            pred_buf[h][...] = part.astype(jnp.bfloat16)
            if merged:
                pair_copy(step).start()
            else:
                for o in order:
                    pred_copy(step, h, o).start()
            parts.append(part)
        if pieces[0][2]:
            pair_copy(step).wait_recv()
            parts[0] = parts[0] + pred_in[0][step, 0].astype(jnp.float32)
            merge_buf[...] = parts[0].astype(jnp.bfloat16)

            @pl.when(inner)
            def _():
                for k in (1, 0):
                    merged_copy(step, k).start()

        grad = None
        for h in [*range(1, len(pieces)), 0] if pieces[0][2] else range(len(pieces)):
            start, width, merged = pieces[h]
            total = meas_ref[:, start:start + width] - parts[h]
            if merged:
                merged_copy(step, 0).wait_recv()
                total = total - pred_in[h][step, 1].astype(jnp.float32)
            else:
                for o in order[::-1]:
                    pred_copy(step, h, o).wait_recv()
                    total = total - pred_in[h][step, o - 1].astype(jnp.float32)
            term = jnp.dot(
                total.astype(jnp.bfloat16), op_ref[start:start + width, :],
                preferred_element_type=jnp.float32,
            )
            grad = term if grad is None else grad + term
        for j in range(n_base):
            grad_buf[j] = grad[:, j * share:(j + 1) * share]
        for o in range(1, n_base):
            grad_copy(step, o).start()
        own = grad_buf[b]
        for o in range(1, n_base):
            grad_copy(step, o).wait_recv()
            own = own + grad_in[step, o - 1]
        return current + descent_stride * own

    def drain(step):
        for h, (_, _, merged) in enumerate(pieces):
            if merged:
                pair_copy(step).wait_send()

                @pl.when(inner)
                def _():
                    for k in (0, 1):
                        merged_copy(step, k).wait_send()
            else:
                for o in order:
                    pred_copy(step, h, o).wait_send()
        for o in range(1, n_base):
            grad_copy(step, o).wait_send()

    for o in range(1, n_base):
        share_copy(sky_ref, 0, o).start()
    first = sky_ref[...]
    xr_buf[b] = first.astype(jnp.bfloat16)
    for o in range(1, n_base):
        share_copy(sky_ref, 0, o).wait()
        xr_buf[base_at(-o)] = z_in[0, o - 1].astype(jnp.bfloat16)
    load.wait()

    def iteration(step, current):
        moved = descend(step, current)
        z_buf[...] = moved
        for o in reversed(range(1, n_base)):
            share_copy(z_buf, step + 1, o).start()
        own_sq = squares(moved)
        sq_buf[...] = own_sq
        for fo in range(1, n_freq):
            for o in reversed(range(n_base)):
                sq_copy(step, fo, o).start()
        drain(step)
        result = None
        for o in range(n_base):
            if o:
                share_copy(z_buf, step + 1, o).wait_recv()
                value = z_in[step + 1, o - 1]
                total = squares(value)
            else:
                value, total = moved, own_sq
            for fo in range(1, n_freq):
                sq_copy(step, fo, o).wait_recv()
                total = total + sq_in[step, (fo - 1) * n_base + o]
            tile = base_at(-o)
            scaled = value * factor_of(step, tile, total)
            xr_buf[tile] = scaled.astype(jnp.bfloat16)
            if o == 0:
                result = scaled
        for o in range(1, n_base):
            share_copy(z_buf, step + 1, o).wait_send()
        for fo in range(1, n_freq):
            for o in range(n_base):
                sq_copy(step, fo, o).wait_send()
        return result

    current = lax.fori_loop(0, ITERS - 1, iteration, first)
    last = ITERS - 1
    moved = descend(last, current)
    total = squares(moved)
    sq_buf[...] = total
    for fo in range(1, n_freq):
        sq_copy(last, fo, 0).start()
    drain(last)
    for fo in range(1, n_freq):
        sq_copy(last, fo, 0).wait()
        total = total + sq_in[last, (fo - 1) * n_base]
    out_ref[...] = moved * factor_of(last, b, total)


def on_device(sensing_operator_parts, sampled_correlations, first_sky_estimate, patch_order_record):
    n_freq, n_base, n_pix = (lax.axis_size(a) for a in ("freq", "base", "pix"))
    chans = sampled_correlations.shape[0]
    share = first_sky_estimate.shape[3]
    op = sensing_operator_parts[0]
    rows, block = op.shape
    f32, bf16 = jnp.float32, jnp.bfloat16
    dma = pltpu.SemaphoreType.DMA
    if n_pix == 4 and rows % 1024 == 0:
        eighth = rows // 8
        pieces = ((0, 3 * eighth, True), (3 * eighth, 2 * eighth, False), (5 * eighth, 3 * eighth, False))
    else:
        pieces = tuple((h * rows // 2, rows // 2, False) for h in range(2))
    piece_scratch = []
    for _, width, _ in pieces:
        piece_scratch += [
            pltpu.VMEM((chans, width), bf16),
            pltpu.VMEM((ITERS, n_pix - 1, chans, width), bf16),
            dma((n_pix - 1,)), dma((ITERS, n_pix - 1)),
        ]
    keep_count = n_base * n_pix // 4
    n_sq = (n_freq - 1) * n_base
    vmem = pl.BlockSpec(memory_space=pltpu.VMEM)
    result = pl.pallas_call(
        functools.partial(kernel, (n_freq, n_base, n_pix, keep_count, pieces)),
        out_shape=jax.ShapeDtypeStruct((chans, share), f32),
        in_specs=[pl.BlockSpec(memory_space=pl.ANY), vmem, vmem, pl.BlockSpec(memory_space=pltpu.SMEM)],
        out_specs=vmem,
        scratch_shapes=[
            pltpu.VMEM((rows, block), bf16),
            pltpu.VMEM((n_base, chans, share), bf16),
            pltpu.VMEM((n_base, chans, share), f32),
            pltpu.VMEM((ITERS, n_base - 1, chans, share), f32),
            pltpu.VMEM((chans, share), f32),
            pltpu.VMEM((ITERS, n_base - 1, chans, share), f32),
            pltpu.VMEM((1, share), f32),
            pltpu.VMEM((ITERS, n_sq, 1, share), f32),
            dma, dma((n_base - 1,)), dma((ITERS, n_base - 1)),
            dma((n_base - 1,)), dma((ITERS, n_base - 1)),
            dma((n_sq,)), dma((ITERS, n_sq)),
            pltpu.VMEM((chans, pieces[0][1]), bf16),
            *piece_scratch,
        ],
        compiler_params=pltpu.CompilerParams(collective_id=0, has_side_effects=True),
    )(op, sampled_correlations, first_sky_estimate.reshape(chans, share), patch_order_record.T)
    return result.reshape(chans, 1, 1, share)


def solution(mesh):
    in_specs = (
        P("freq", "base", "pix"),
        P("freq", "base"),
        P("freq", "pix", "base", None),
        P(None, "pix"),
    )
    out_specs = P("freq", "pix", "base", None)
    return jax.shard_map(
        on_device, mesh=mesh, in_specs=in_specs, out_specs=out_specs, check_vma=False
    )
```
